32 devices in a mesh: row: 4 (over x, core), col: 8 (over z, y).
Axes of the slice: x: 2, y: 2, z: 4, core: 2. Of those that a mesh axis runs over, the one named last changes fastest.
Arguments:
- edge_h: int32 [128, 1024], P('row', 'col'), may hold values from 0 to 7
- edge_v: int32 [128, 1024], P('row', 'col'), may hold values from 0 to 7
- pads: int32 [128, 1024], P('row', 'col'), may hold values 0 or 1
- loads: int32 [256, 128, 1024], P(None, 'row', 'col'), may hold values from 0 to 7
- scales: float32 [256, 8], replicated, may hold values from 0.25 to 4
Outputs:
- drop: float32 [256, 128, 1024], P(None, 'row', 'col')
- res_norms: float32 [256, 5], replicated
The draws below stay inside these ranges and needn't reach their ends.
All inputs are finite; a program needn't handle non-finite values. No bound on the sum of `pads` on one device may be relied on, other than what follows from the above.
Results may differ from the reference program's by a relative error of at most 0.0003.
Values sent between devices are 32-bit elements; how exact they have to be, the bound alone decides.
A program may use at most 128 MiB of HBM per device.

```python
import math
import jax
import jax.numpy as jnp
from jax import lax

SCEN = 256
ITERS = 4
NR = 128
NC = 1024


def plant(entries, key, least, high):
    shape = entries.shape
    spot = [jax.random.randint(jax.random.fold_in(key, axis), (), 0, shape[axis]) for axis in range(len(shape))]
    entries = entries.at[tuple(spot)].set(least)
    longest = shape.index(max(shape))
    spot[longest] = (spot[longest] + 1) % shape[longest]
    return entries.at[tuple(spot)].set(high)


def setup_inputs(seed: int = 0) -> dict:
    streams_of = jax.random.split(jax.random.key(seed), 6)
    edge_h = plant(jax.random.randint(streams_of[0], (NR, NC), 0, 8), jax.random.fold_in(streams_of[0], 1), 0, 7).astype(jnp.int32)
    edge_v = plant(jax.random.randint(streams_of[1], (NR, NC), 0, 8), jax.random.fold_in(streams_of[1], 1), 0, 7).astype(jnp.int32)
    pads = plant((jax.random.randint(streams_of[2], (NR, NC), 0, 16) < 1).astype(jnp.int32), jax.random.fold_in(streams_of[2], 1), 0, 1)
    loads = plant(jax.random.randint(streams_of[3], (SCEN, NR, NC), 0, 8), jax.random.fold_in(streams_of[3], 1), 0, 7).astype(jnp.int32)
    scales = jnp.clip(jnp.exp(jax.random.uniform(streams_of[4], (SCEN, 8), jnp.float32, math.log(0.25), math.log(4.0))), 0.25, 4.0)
    return dict(edge_h=edge_h, edge_v=edge_v, pads=pads, loads=loads, scales=scales)


edge_table = (0.5, 0.8, 1.2, 1.7, 2.3, 3.0, 3.8, 4.7)
load_table = (0.25, 0.5, 1.0, 1.5, 2.0, 3.0, 4.0, 6.0)
pad_conductance = 20.0
leakage = 0.05

def lookup(classes, table):
    total = jnp.zeros(classes.shape, jnp.float32)
    for number, amount in enumerate(table):
        total = total + jnp.where(classes == number, jnp.float32(amount), jnp.float32(0.0))
    return total

def apply_grid(field, g_east, g_west, g_south, g_north, diagonal):
    padded = jnp.pad(field, 1)
    north = padded[:-2, 1:-1]
    south = padded[2:, 1:-1]
    west = padded[1:-1, :-2]
    east = padded[1:-1, 2:]
    return diagonal * field - (g_east * east + g_west * west + g_south * south + g_north * north)

def reference(edge_h, edge_v, pads, loads, scales):
    rows_all, cols_all = pads.shape
    row_ids = lax.broadcasted_iota(jnp.int32, pads.shape, 0)
    col_ids = lax.broadcasted_iota(jnp.int32, pads.shape, 1)
    zero = jnp.zeros(pads.shape, jnp.float32)
    g_east = jnp.where(col_ids < cols_all - 1, lookup(edge_h, edge_table), zero)
    g_south = jnp.where(row_ids < rows_all - 1, lookup(edge_v, edge_table), zero)
    g_west = jnp.pad(g_east[:, :-1], ((0, 0), (1, 0)))
    g_north = jnp.pad(g_south[:-1], ((1, 0), (0, 0)))
    diagonal = g_east + g_west + g_south + g_north + pads.astype(jnp.float32) * pad_conductance + leakage
    weights = -scales.astype(jnp.float32) * jnp.asarray(load_table, jnp.float32)[None, :]

    def solve_one(pair):
        weight_row, load_map = pair
        right = jnp.zeros(load_map.shape, jnp.float32)
        for number in range(8):
            right = right + jnp.where(load_map == number, weight_row[number], jnp.float32(0.0))
        solution = jnp.zeros_like(right)
        resid = right
        precond = resid / diagonal
        direction = precond
        gamma = jnp.sum(resid * precond)
        norms = [jnp.sqrt(jnp.sum(resid * resid))]
        for iteration in range(ITERS):
            image = apply_grid(direction, g_east, g_west, g_south, g_north, diagonal)
            alpha = gamma / jnp.sum(direction * image)
            solution = solution + alpha * direction
            resid = resid - alpha * image
            precond = resid / diagonal
            gamma_new = jnp.sum(resid * precond)
            norms.append(jnp.sqrt(jnp.sum(resid * resid)))
            direction = precond + gamma_new / gamma * direction
            gamma = gamma_new
        return (solution, jnp.stack(norms))
    drop, res_norms = lax.map(solve_one, (weights, loads))
    return (drop, res_norms)
```

```python
import functools

import jax
import jax.numpy as jnp
from jax import lax
from jax.experimental import pallas as pl
from jax.experimental.pallas import tpu as pltpu
from jax.sharding import PartitionSpec as P

ITERS = 4
H = ITERS
LANES = 128
MESH = pl.DeviceIdType.MESH

edge_table = (0.5, 0.8, 1.2, 1.7, 2.3, 3.0, 3.8, 4.7)
load_table = (0.25, 0.5, 1.0, 1.5, 2.0, 3.0, 4.0, 6.0)
pad_conductance = 20.0
leakage = 0.05

DIRS = [(-1, 0), (1, 0), (0, -1), (0, 1), (-1, -1), (-1, 1), (1, -1), (1, 1)]
MOMENTS = [(m // 2, m - m // 2) for m in range(2 * ITERS)]
GRAM = [(i, j) for i in range(ITERS + 1) for j in range(i, ITERS + 1)]
SUMS = len(MOMENTS) + len(GRAM)
SLOTS = -(-SUMS // 8) * 8


def lookup_edge(classes):
    total = jnp.zeros(classes.shape, jnp.float32)
    for number, amount in enumerate(edge_table):
        total = jnp.where(classes == number, jnp.float32(amount), total)
    return total


def pick(classes, rows):
    low = (classes & 1) == 0
    mid = (classes & 2) == 0
    high = (classes & 4) == 0
    a = [jnp.where(low, rows[2 * i], rows[2 * i + 1]) for i in range(4)]
    b = [jnp.where(mid, a[0], a[1]), jnp.where(mid, a[2], a[3])]
    return jnp.where(high, b[0], b[1])


def kernel(
    nr, nc, maps, loads, weights, drop, norms,
    rowbuf, colbuf, corner, mrow, mcol, mcorner,
    z, gE, gW, gS, gN, diag, recip, acc, part, slots_row, mid, slots_col, coef,
    send_sem, recv_sem, send_row, recv_row, send_col, recv_col,
):
    halves, rows, cols, _ = loads.shape
    ext_r, ext_c = rows + 2 * H, cols + 8
    me_r, me_c = lax.axis_index("row"), lax.axis_index("col")

    def exists(dr, dc):
        r, c = me_r + dr, me_c + dc
        return (r >= 0) & (r < nr) & (c >= 0) & (c < nc)

    def side(d):
        return 0 if d < 0 else 1

    def load_copy(k):
        dr, dc = DIRS[k]
        rs = pl.ds(0, H) if dr < 0 else pl.ds(rows - H, H)
        cs = pl.ds(0, 8) if dc < 0 else pl.ds(cols - 8, 8)
        if dc == 0:
            src, dst = loads.at[:, rs], rowbuf.at[side(-dr)]
        elif dr == 0:
            src, dst = loads.at[:, :, cs], colbuf.at[side(-dc)]
        else:
            src, dst = loads.at[:, rs, cs], corner.at[2 * side(-dr) + side(-dc)]
        return pltpu.make_async_remote_copy(
            src_ref=src, dst_ref=dst, send_sem=send_sem.at[k], recv_sem=recv_sem.at[k],
            device_id=(me_r + dr, me_c + dc), device_id_type=MESH,
        )

    def map_copy(k):
        dr, dc = DIRS[k]
        rs = pl.ds(0, 8) if dr < 0 else pl.ds(rows - 8, 8)
        if dc == 0:
            src, dst = maps.at[:, rs], mrow.at[side(-dr)]
        elif dr == 0:
            src, dst = maps, mcol.at[side(-dc)]
        else:
            src, dst = maps.at[:, rs], mcorner.at[2 * side(-dr) + side(-dc)]
        return pltpu.make_async_remote_copy(
            src_ref=src, dst_ref=dst, send_sem=send_sem.at[8 + k], recv_sem=recv_sem.at[8 + k],
            device_id=(me_r + dr, me_c + dc), device_id_type=MESH,
        )

    barrier = pltpu.get_barrier_semaphore()
    for j in range(1, nr):
        pl.semaphore_signal(
            barrier, inc=1, device_id=(lax.rem(me_r + j, nr), me_c), device_id_type=MESH
        )
    for j in range(1, nc):
        pl.semaphore_signal(
            barrier, inc=1, device_id=(me_r, lax.rem(me_c + j, nc)), device_id_type=MESH
        )
    for dr, dc in DIRS[4:]:
        corner_id = (lax.rem(me_r + dr + nr, nr), lax.rem(me_c + dc + nc, nc))
        pl.semaphore_signal(barrier, inc=1, device_id=corner_id, device_id_type=MESH)
    pl.semaphore_wait(barrier, nr + nc - 2 + 4)

    for k in range(8):

        @pl.when(exists(*DIRS[k]))
        def _():
            map_copy(k).start()

    for k in range(8):

        @pl.when(exists(*DIRS[k]))
        def _():
            load_copy(k).start()

    for k in range(8):

        @pl.when(exists(-DIRS[k][0], -DIRS[k][1]))
        def _():
            map_copy(k).wait_recv()

    pad_rows = jnp.zeros((LANES - ext_r - 1, cols), jnp.float32)

    def stretch(north, own, south):
        tall = jnp.concatenate([north[8 - H :], own, south[:H]], axis=0).astype(jnp.float32)
        before = north[7 - H : 8 - H].astype(jnp.float32)
        return jnp.concatenate([tall, pad_rows, before], axis=0).T

    sub8 = lax.broadcasted_iota(jnp.int32, (8, LANES), 0)

    def widened(m):
        own = stretch(mrow[0, m], maps[m], mrow[1, m])
        west = stretch(mcorner[0, m], mcol[0, m], mcorner[2, m])
        east = stretch(mcorner[1, m], mcol[1, m], mcorner[3, m])
        rim = jnp.where(sub8 < H, east[:8], west[cols - 8 :])
        return jnp.concatenate([own, rim], axis=0), west[cols - 8 :]

    sub = lax.broadcasted_iota(jnp.int32, (ext_c, LANES), 0)
    lane = lax.broadcasted_iota(jnp.int32, (ext_c, LANES), 1)
    col_id = me_c * cols + jnp.where(sub >= cols + H, sub - ext_c, sub)
    row_id = me_r * rows + jnp.where(lane == LANES - 1, -1, lane) - H
    east_class, west_class = widened(0)
    e = jnp.where((col_id >= 0) & (col_id < nc * cols - 1), lookup_edge(east_class), 0.0)
    s = jnp.where((row_id >= 0) & (row_id < nr * rows - 1), lookup_edge(widened(1)[0]), 0.0)
    w = pltpu.roll(e, 1, 0)
    beyond = jnp.where(me_c > 0, lookup_edge(west_class), 0.0)
    rim_w = jnp.where(sub8 < H, w[cols:], pltpu.roll(beyond, 1, 0))
    w = jnp.concatenate([w[:cols], rim_w], axis=0)
    n = pltpu.roll(s, 1, 1)
    d = e + w + s + n + jnp.where(widened(2)[0] == 1.0, pad_conductance, 0.0) + leakage
    inv = 1.0 / d
    inv = inv * (2.0 - d * inv)
    inv = inv * (2.0 - d * inv)
    for ref, value in (
        (gE, e * inv), (gW, w * inv), (gS, s * inv), (gN, n * inv), (diag, d), (recip, inv)
    ):
        for r in range(ext_r):
            ref[r] = jnp.broadcast_to(value[:, r : r + 1], (ext_c, LANES))

    wrows = [[weights[h, c : c + 1, :] for c in range(8)] for h in range(halves)]

    @pl.loop(0, rows)
    def _(r):
        for h in range(halves):
            z[0, h, r + H, :cols] = pick(loads[h, r], wrows[h]) * recip[r + H, :cols]

    for k in range(8):

        @pl.when(exists(-DIRS[k][0], -DIRS[k][1]))
        def _():
            load_copy(k).wait_recv()

    @pl.loop(0, rows)
    def _(r):
        for h in range(halves):
            rim = jnp.where(sub8 < H, colbuf[1, h, r], colbuf[0, h, r])
            z[0, h, r + H, cols:] = pick(rim, wrows[h]) * recip[r + H, cols:]

    @pl.loop(0, H)
    def _(i):
        for h in range(halves):
            for q, base in ((0, 0), (1, rows + H)):
                r = base + i
                z[0, h, r, :cols] = pick(rowbuf[q, h, i], wrows[h]) * recip[r, :cols]
                rim = jnp.where(sub8 < H, corner[2 * q + 1, h, i], corner[2 * q, h, i])
                z[0, h, r, cols:] = pick(rim, wrows[h]) * recip[r, cols:]

    for k in range(ITERS):

        @pl.loop(k + 1, ext_r - k - 1)
        def _(r):
            for h in range(halves):
                centre = z[k, h, r]
                z[k + 1, h, r] = (
                    gE[r] * pltpu.roll(centre, ext_c - 1, 0)
                    + gW[r] * pltpu.roll(centre, 1, 0)
                ) + (gS[r] * z[k, h, r + 1] + gN[r] * z[k, h, r - 1])

    acc[...] = jnp.zeros_like(acc)
    for h in range(halves):

        @pl.loop(H, rows + H)
        def _(r):
            totals = None
            for t in range(cols // 8):
                at = pl.ds(8 * t, 8)
                zs = [z[i, h, r, at] for i in range(ITERS + 1)]
                dd = diag[r, at]
                vs = [dd * x for x in zs]
                terms = [zs[i] * vs[j] for i, j in MOMENTS] + [vs[i] * vs[j] for i, j in GRAM]
                totals = terms if totals is None else [a + b for a, b in zip(totals, terms)]
            for i, total in enumerate(totals):
                acc[h, i] += total

    for h in range(halves):
        for i in range(SLOTS):
            part[h, i : i + 1] = jnp.sum(acc[h, i], axis=0, keepdims=True)

    def share(src, slots, me, count, axis, sends, recvs):
        def copy(j):
            other = lax.rem(me + j, count)
            target = (other, me_c) if axis == "row" else (me_r, other)
            return pltpu.make_async_remote_copy(
                src_ref=src, dst_ref=slots.at[me], send_sem=sends.at[j], recv_sem=recvs.at[j],
                device_id=target, device_id_type=MESH,
            )

        slots[me] = src[...]
        for j in range(1, count):
            copy(j).start()
        for j in range(1, count):
            copy(j).wait_recv()
        for j in range(1, count):
            copy(j).wait_send()
        total = slots[0]
        for i in range(1, count):
            total = total + slots[i]
        return total

    mid[...] = share(part, slots_row, me_r, nr, "row", send_row, recv_row)
    coef[...] = share(mid, slots_col, me_c, nc, "col", send_col, recv_col)

    def row_of(i):
        return coef[:, i, :]

    moment = [row_of(i) for i in range(len(MOMENTS))]
    gram = {pair: row_of(len(MOMENTS) + i) for i, pair in enumerate(GRAM)}
    zero = jnp.zeros_like(moment[0])
    one = jnp.ones_like(moment[0])

    def energy(a):
        total = None
        for i in range(len(a)):
            for j in range(len(a)):
                term = a[i] * a[j] * moment[i + j]
                total = term if total is None else total + term
        return total

    def stiffness(b):
        total = None
        for i in range(len(b)):
            for j in range(len(b)):
                term = b[i] * b[j] * (moment[i + j] - moment[i + j + 1])
                total = term if total is None else total + term
        return total

    def square(a):
        total = None
        for i in range(len(a)):
            for j in range(i, len(a)):
                term = a[i] * a[j] * gram[i, j]
                term = term if i == j else 2.0 * term
                total = term if total is None else total + term
        return jnp.sqrt(jnp.maximum(total, 0.0))

    resid, direction, answer = [one], [one], []
    gamma = moment[0]
    results = [square(resid)]
    for k in range(ITERS):
        alpha = gamma / stiffness(direction)
        answer = [
            (answer[i] if i < len(answer) else zero) + alpha * direction[i]
            for i in range(len(direction))
        ]
        image = [
            (direction[i] if i < len(direction) else zero)
            - (direction[i - 1] if i > 0 else zero)
            for i in range(len(direction) + 1)
        ]
        resid = [
            (resid[i] if i < len(resid) else zero) - alpha * image[i] for i in range(len(image))
        ]
        results.append(square(resid))
        if k + 1 < ITERS:
            gamma_new = energy(resid)
            ratio = gamma_new / gamma
            direction = [
                resid[i] + (ratio * direction[i] if i < len(direction) else zero)
                for i in range(len(resid))
            ]
            gamma = gamma_new
    for i, value in enumerate(results):
        norms[:, i, :] = value
    for i in range(ITERS + 1, norms.shape[1]):
        norms[:, i, :] = zero

    for h in range(halves):
        scale = [answer[i][h : h + 1] for i in range(ITERS)]

        @pl.loop(0, rows)
        def _(r):
            total = scale[0] * z[0, h, r + H, :cols]
            for i in range(1, ITERS):
                total = total + scale[i] * z[i, h, r + H, :cols]
            drop[h, r] = total

    for k in range(8):

        @pl.when(exists(*DIRS[k]))
        def _():
            map_copy(k).wait_send()
            load_copy(k).wait_send()


def local(nr, nc, edge_h, edge_v, pads, loads, scales):
    scen, rows, cols = loads.shape
    halves = scen // LANES
    weights = -scales * jnp.asarray(load_table, jnp.float32)[None, :]
    weights = weights.reshape(halves, LANES, 8).transpose(0, 2, 1)
    maps = jnp.stack([edge_h, edge_v, pads])
    turned = loads.reshape(halves, LANES, rows, cols).transpose(0, 2, 3, 1)
    ext_r, ext_c = rows + 2 * H, cols + 8
    f32, i32 = jnp.float32, jnp.int32
    norm_rows = -(-(ITERS + 1) // 8) * 8
    vmem = pl.BlockSpec(memory_space=pltpu.VMEM)
    dma = pltpu.SemaphoreType.DMA
    drop, norms = pl.pallas_call(
        functools.partial(kernel, nr, nc),
        out_shape=(
            jax.ShapeDtypeStruct((halves, rows, cols, LANES), f32),
            jax.ShapeDtypeStruct((halves, norm_rows, LANES), f32),
        ),
        in_specs=[vmem] * 3,
        out_specs=(vmem, vmem),
        scratch_shapes=[
            pltpu.VMEM((2, halves, H, cols, LANES), i32),
            pltpu.VMEM((2, halves, rows, 8, LANES), i32),
            pltpu.VMEM((4, halves, H, 8, LANES), i32),
            pltpu.VMEM((2, 3, 8, cols), i32),
            pltpu.VMEM((2, 3, rows, cols), i32),
            pltpu.VMEM((4, 3, 8, cols), i32),
            pltpu.VMEM((ITERS + 1, halves, ext_r, ext_c, LANES), f32),
            *[pltpu.VMEM((ext_r, ext_c, LANES), f32) for _ in range(6)],
            pltpu.VMEM((halves, SLOTS, 8, LANES), f32),
            pltpu.VMEM((halves, SLOTS, LANES), f32),
            pltpu.VMEM((nr, halves, SLOTS, LANES), f32),
            pltpu.VMEM((halves, SLOTS, LANES), f32),
            pltpu.VMEM((nc, halves, SLOTS, LANES), f32),
            pltpu.VMEM((halves, SLOTS, LANES), f32),
            dma((16,)),
            dma((16,)),
            dma((nr,)),
            dma((nr,)),
            dma((nc,)),
            dma((nc,)),
        ],
        compiler_params=pltpu.CompilerParams(
            collective_id=0, has_side_effects=True, vmem_limit_bytes=67043328
        ),
        name="grid_cg",
    )(maps, turned, weights)
    drop = drop.transpose(0, 3, 1, 2).reshape(scen, rows, cols)
    norms = norms.transpose(0, 2, 1).reshape(scen, norm_rows)[:, : ITERS + 1]
    return drop, norms


def solution(mesh):
    return jax.shard_map(
        functools.partial(local, mesh.shape["row"], mesh.shape["col"]),
        mesh=mesh,
        in_specs=(P("row", "col"), P("row", "col"), P("row", "col"), P(None, "row", "col"), P()),
        out_specs=(P(None, "row", "col"), P()),
        check_vma=False,
    )
```

```python
import functools

import jax
import jax.numpy as jnp
from jax import lax
from jax.experimental import pallas as pl
from jax.experimental.pallas import tpu as pltpu
from jax.sharding import PartitionSpec as P

ITERS = 4
H = ITERS
LANES = 128
MESH = pl.DeviceIdType.MESH

edge_table = (0.5, 0.8, 1.2, 1.7, 2.3, 3.0, 3.8, 4.7)
load_table = (0.25, 0.5, 1.0, 1.5, 2.0, 3.0, 4.0, 6.0)
pad_conductance = 20.0
leakage = 0.05

DIRS = [(-1, 0), (1, 0), (0, -1), (0, 1), (-1, -1), (-1, 1), (1, -1), (1, 1)]
LAST = ITERS - 1
MU = 0
NU = 1
EP = NU + ITERS
KA = EP + 2 * ITERS - 2
VV = KA + 2 * ITERS - 3
VW = VV + 1
WW = VW + ITERS
PAIRS = [(i, j) for i in range(ITERS) for j in range(i, ITERS)]
SUMS = WW + len(PAIRS)
SLOTS = -(-SUMS // 8) * 8


def lookup_edge(classes):
    total = jnp.zeros(classes.shape, jnp.float32)
    for number, amount in enumerate(edge_table):
        total = jnp.where(classes == number, jnp.float32(amount), total)
    return total


def pick(classes, rows):
    low = (classes & 1) == 0
    mid = (classes & 2) == 0
    high = (classes & 4) == 0
    a = [jnp.where(low, rows[2 * i], rows[2 * i + 1]) for i in range(4)]
    b = [jnp.where(mid, a[0], a[1]), jnp.where(mid, a[2], a[3])]
    return jnp.where(high, b[0], b[1])


def kernel(
    nr, nc, maps, loads, weights, drop, norms,
    rowbuf, colbuf, corner, mrow, mcol, mcorner,
    z, gE, gW, gS, gN, diag, recip, acc, part, slots_row, mid, slots_col, coef,
    send_sem, recv_sem, send_row, recv_row, send_col, recv_col,
):
    halves, rows, cols, _ = loads.shape
    ext_r, ext_c = rows + 2 * H, cols + 8
    me_r, me_c = lax.axis_index("row"), lax.axis_index("col")

    def exists(dr, dc):
        r, c = me_r + dr, me_c + dc
        return (r >= 0) & (r < nr) & (c >= 0) & (c < nc)

    def side(d):
        return 0 if d < 0 else 1

    def load_copy(k):
        dr, dc = DIRS[k]
        rs = pl.ds(0, H) if dr < 0 else pl.ds(rows - H, H)
        cs = pl.ds(0, 8) if dc < 0 else pl.ds(cols - 8, 8)
        if dc == 0:
            src, dst = loads.at[:, rs], rowbuf.at[side(-dr)]
        elif dr == 0:
            src, dst = loads.at[:, :, cs], colbuf.at[side(-dc)]
        else:
            src, dst = loads.at[:, rs, cs], corner.at[2 * side(-dr) + side(-dc)]
        return pltpu.make_async_remote_copy(
            src_ref=src, dst_ref=dst, send_sem=send_sem.at[k], recv_sem=recv_sem.at[k],
            device_id=(me_r + dr, me_c + dc), device_id_type=MESH,
        )

    def map_copy(k):
        dr, dc = DIRS[k]
        rs = pl.ds(0, 8) if dr < 0 else pl.ds(rows - 8, 8)
        if dc == 0:
            src, dst = maps.at[:, rs], mrow.at[side(-dr)]
        elif dr == 0:
            src, dst = maps, mcol.at[side(-dc)]
        else:
            src, dst = maps.at[:, rs], mcorner.at[2 * side(-dr) + side(-dc)]
        return pltpu.make_async_remote_copy(
            src_ref=src, dst_ref=dst, send_sem=send_sem.at[8 + k], recv_sem=recv_sem.at[8 + k],
            device_id=(me_r + dr, me_c + dc), device_id_type=MESH,
        )

    barrier = pltpu.get_barrier_semaphore()
    for j in range(1, nr):
        pl.semaphore_signal(
            barrier, inc=1, device_id=(lax.rem(me_r + j, nr), me_c), device_id_type=MESH
        )
    for j in range(1, nc):
        pl.semaphore_signal(
            barrier, inc=1, device_id=(me_r, lax.rem(me_c + j, nc)), device_id_type=MESH
        )
    for dr, dc in DIRS[4:]:
        corner_id = (lax.rem(me_r + dr + nr, nr), lax.rem(me_c + dc + nc, nc))
        pl.semaphore_signal(barrier, inc=1, device_id=corner_id, device_id_type=MESH)
    pl.semaphore_wait(barrier, nr + nc - 2 + 4)

    for k in range(8):

        @pl.when(exists(*DIRS[k]))
        def _():
            map_copy(k).start()

    for k in range(8):

        @pl.when(exists(*DIRS[k]))
        def _():
            load_copy(k).start()

    for k in range(8):

        @pl.when(exists(-DIRS[k][0], -DIRS[k][1]))
        def _():
            map_copy(k).wait_recv()

    pad_rows = jnp.zeros((LANES - ext_r - 1, cols), jnp.float32)

    def stretch(north, own, south):
        tall = jnp.concatenate([north[8 - H :], own, south[:H]], axis=0).astype(jnp.float32)
        before = north[7 - H : 8 - H].astype(jnp.float32)
        return jnp.concatenate([tall, pad_rows, before], axis=0).T

    sub8 = lax.broadcasted_iota(jnp.int32, (8, LANES), 0)

    def widened(m):
        own = stretch(mrow[0, m], maps[m], mrow[1, m])
        west = stretch(mcorner[0, m], mcol[0, m], mcorner[2, m])
        east = stretch(mcorner[1, m], mcol[1, m], mcorner[3, m])
        rim = jnp.where(sub8 < H, east[:8], west[cols - 8 :])
        return jnp.concatenate([own, rim], axis=0), west[cols - 8 :]

    sub = lax.broadcasted_iota(jnp.int32, (ext_c, LANES), 0)
    lane = lax.broadcasted_iota(jnp.int32, (ext_c, LANES), 1)
    col_id = me_c * cols + jnp.where(sub >= cols + H, sub - ext_c, sub)
    row_id = me_r * rows + jnp.where(lane == LANES - 1, -1, lane) - H
    east_class, west_class = widened(0)
    e = jnp.where((col_id >= 0) & (col_id < nc * cols - 1), lookup_edge(east_class), 0.0)
    s = jnp.where((row_id >= 0) & (row_id < nr * rows - 1), lookup_edge(widened(1)[0]), 0.0)
    w = pltpu.roll(e, 1, 0)
    beyond = jnp.where(me_c > 0, lookup_edge(west_class), 0.0)
    rim_w = jnp.where(sub8 < H, w[cols:], pltpu.roll(beyond, 1, 0))
    w = jnp.concatenate([w[:cols], rim_w], axis=0)
    n = pltpu.roll(s, 1, 1)
    d = e + w + s + n + jnp.where(widened(2)[0] == 1.0, pad_conductance, 0.0) + leakage
    inv = 1.0 / d
    inv = inv * (2.0 - d * inv)
    inv = inv * (2.0 - d * inv)
    for ref, value in (
        (gE, e * inv), (gW, w * inv), (gS, s * inv), (gN, n * inv), (diag, d), (recip, inv)
    ):
        for r in range(ext_r):
            ref[r] = jnp.broadcast_to(value[:, r : r + 1], (ext_c, LANES))

    wrows = [[weights[h, c : c + 1, :] for c in range(8)] for h in range(halves)]

    @pl.loop(0, rows)
    def _(r):
        for h in range(halves):
            z[0, h, r + H, :cols] = pick(loads[h, r], wrows[h]) * recip[r + H, :cols]

    for k in range(8):

        @pl.when(exists(-DIRS[k][0], -DIRS[k][1]))
        def _():
            load_copy(k).wait_recv()

    @pl.loop(0, rows)
    def _(r):
        for h in range(halves):
            rim = jnp.where(sub8 < H, colbuf[1, h, r], colbuf[0, h, r])
            z[0, h, r + H, cols:] = pick(rim, wrows[h]) * recip[r + H, cols:]

    @pl.loop(0, H)
    def _(i):
        for h in range(halves):
            for q, base in ((0, 0), (1, rows + H)):
                r = base + i
                z[0, h, r, :cols] = pick(rowbuf[q, h, i], wrows[h]) * recip[r, :cols]
                rim = jnp.where(sub8 < H, corner[2 * q + 1, h, i], corner[2 * q, h, i])
                z[0, h, r, cols:] = pick(rim, wrows[h]) * recip[r, cols:]

    for k in range(ITERS):

        @pl.loop(k + 1, ext_r - k - 1)
        def _(r):
            for h in range(halves):
                centre = z[k, h, r]
                z[k + 1, h, r] = (
                    gE[r] * pltpu.roll(centre, ext_c - 1, 0)
                    + gW[r] * pltpu.roll(centre, 1, 0)
                ) + (gS[r] * z[k, h, r + 1] + gN[r] * z[k, h, r - 1])

    acc[...] = jnp.zeros_like(acc)
    for h in range(halves):

        @pl.loop(H, rows + H)
        def _(r):
            totals = None
            for t in range(cols // 8):
                at = pl.ds(8 * t, 8)
                zs = [z[i, h, r, at] for i in range(ITERS + 1)]
                dd = diag[r, at]
                es = [zs[i] - zs[i + 1] for i in range(ITERS)]
                fs = [es[i] - es[i + 1] for i in range(LAST)]
                ws = [dd * e for e in es]
                top = dd * zs[ITERS]
                terms = [zs[LAST] * (dd * zs[LAST])]
                terms += [zs[LAST] * ws[i] for i in range(ITERS)]
                terms += [es[m // 2] * ws[m - m // 2] for m in range(2 * ITERS - 2)]
                terms += [fs[m // 2] * ws[m - m // 2] for m in range(2 * ITERS - 3)]
                terms += [top * top] + [top * ws[i] for i in range(ITERS)]
                terms += [ws[i] * ws[j] for i, j in PAIRS]
                totals = terms if totals is None else [a + b for a, b in zip(totals, terms)]
            for i, total in enumerate(totals):
                acc[h, i] += total

    for h in range(halves):
        for i in range(SLOTS):
            part[h, i : i + 1] = jnp.sum(acc[h, i], axis=0, keepdims=True)

    def share(src, slots, me, count, axis, sends, recvs):
        def copy(j):
            other = lax.rem(me + j, count)
            target = (other, me_c) if axis == "row" else (me_r, other)
            return pltpu.make_async_remote_copy(
                src_ref=src, dst_ref=slots.at[me], send_sem=sends.at[j], recv_sem=recvs.at[j],
                device_id=target, device_id_type=MESH,
            )

        slots[me] = src[...]
        for j in range(1, count):
            copy(j).start()
        for j in range(1, count):
            copy(j).wait_recv()
        for j in range(1, count):
            copy(j).wait_send()
        total = slots[0]
        for i in range(1, count):
            total = total + slots[i]
        return total

    mid[...] = share(part, slots_row, me_r, nr, "row", send_row, recv_row)
    coef[...] = share(mid, slots_col, me_c, nc, "col", send_col, recv_col)

    def row_of(i):
        return coef[:, i, :]

    zero = jnp.zeros_like(row_of(0))
    one = jnp.ones_like(zero)
    cross = {pair: row_of(WW + i) for i, pair in enumerate(PAIRS)}

    def quadratic(a, entry):
        total = None
        for i in range(len(a)):
            for j in range(i, len(a)):
                term = a[i] * a[j] * entry(i, j)
                term = term if i == j else 2.0 * term
                total = term if total is None else total + term
        return total

    def energy(c):
        edge = sum(c[i] * row_of(NU + i) for i in range(LAST))
        return row_of(MU) + 2.0 * edge + quadratic(c[:LAST], lambda i, j: row_of(EP + i + j))

    def stiffness(s, b):
        edge = sum(b[i] * row_of(EP + LAST + i) for i in range(LAST))
        inner = quadratic(b, lambda i, j: row_of(KA + i + j))
        return s * (s * row_of(NU + LAST) + 2.0 * edge) + inner

    def norm(c):
        edge = sum(c[i] * row_of(VW + i) for i in range(ITERS))
        total = row_of(VV) + 2.0 * edge + quadratic(c, lambda i, j: cross[i, j])
        return jnp.sqrt(jnp.maximum(total, 0.0))

    c, s_top, b = [one] * ITERS, one, [one] * LAST
    answer = [zero] * ITERS
    gamma = energy(c)
    results = [norm(c)]
    for k in range(ITERS):
        alpha = gamma / stiffness(s_top, b)
        ends = [zero] + b + [s_top]
        for i in range(k + 1):
            step = alpha * (ends[i + 1] - ends[i])
            answer[i] = answer[i] + step
            c[i] = c[i] - step
        results.append(norm(c))
        if k + 1 < ITERS:
            gamma_new = energy(c)
            ratio = gamma_new / gamma
            s_top = 1.0 + ratio * s_top
            b = [c[i] + ratio * b[i] for i in range(LAST)]
            gamma = gamma_new
    for i, value in enumerate(results):
        norms[:, i, :] = value
    for i in range(ITERS + 1, norms.shape[1]):
        norms[:, i, :] = zero

    for h in range(halves):
        scale = [answer[i][h : h + 1] for i in range(ITERS)]

        @pl.loop(0, rows)
        def _(r):
            total = scale[0] * z[0, h, r + H, :cols]
            for i in range(1, ITERS):
                total = total + scale[i] * z[i, h, r + H, :cols]
            drop[h, r] = total

    for k in range(8):

        @pl.when(exists(*DIRS[k]))
        def _():
            map_copy(k).wait_send()
            load_copy(k).wait_send()


def local(nr, nc, edge_h, edge_v, pads, loads, scales):
    scen, rows, cols = loads.shape
    halves = scen // LANES
    weights = -scales * jnp.asarray(load_table, jnp.float32)[None, :]
    weights = weights.reshape(halves, LANES, 8).transpose(0, 2, 1)
    maps = jnp.stack([edge_h, edge_v, pads])
    turned = loads.reshape(halves, LANES, rows, cols).transpose(0, 2, 3, 1)
    ext_r, ext_c = rows + 2 * H, cols + 8
    f32, i32 = jnp.float32, jnp.int32
    norm_rows = -(-(ITERS + 1) // 8) * 8
    vmem = pl.BlockSpec(memory_space=pltpu.VMEM)
    dma = pltpu.SemaphoreType.DMA
    drop, norms = pl.pallas_call(
        functools.partial(kernel, nr, nc),
        out_shape=(
            jax.ShapeDtypeStruct((halves, rows, cols, LANES), f32),
            jax.ShapeDtypeStruct((halves, norm_rows, LANES), f32),
        ),
        in_specs=[vmem] * 3,
        out_specs=(vmem, vmem),
        scratch_shapes=[
            pltpu.VMEM((2, halves, H, cols, LANES), i32),
            pltpu.VMEM((2, halves, rows, 8, LANES), i32),
            pltpu.VMEM((4, halves, H, 8, LANES), i32),
            pltpu.VMEM((2, 3, 8, cols), i32),
            pltpu.VMEM((2, 3, rows, cols), i32),
            pltpu.VMEM((4, 3, 8, cols), i32),
            pltpu.VMEM((ITERS + 1, halves, ext_r, ext_c, LANES), f32),
            *[pltpu.VMEM((ext_r, ext_c, LANES), f32) for _ in range(6)],
            pltpu.VMEM((halves, SLOTS, 8, LANES), f32),
            pltpu.VMEM((halves, SLOTS, LANES), f32),
            pltpu.VMEM((nr, halves, SLOTS, LANES), f32),
            pltpu.VMEM((halves, SLOTS, LANES), f32),
            pltpu.VMEM((nc, halves, SLOTS, LANES), f32),
            pltpu.VMEM((halves, SLOTS, LANES), f32),
            dma((16,)),
            dma((16,)),
            dma((nr,)),
            dma((nr,)),
            dma((nc,)),
            dma((nc,)),
        ],
        compiler_params=pltpu.CompilerParams(
            collective_id=0, has_side_effects=True, vmem_limit_bytes=67043328
        ),
        name="grid_cg",
    )(maps, turned, weights)
    drop = drop.transpose(0, 3, 1, 2).reshape(scen, rows, cols)
    norms = norms.transpose(0, 2, 1).reshape(scen, norm_rows)[:, : ITERS + 1]
    return drop, norms


def solution(mesh):
    return jax.shard_map(
        functools.partial(local, mesh.shape["row"], mesh.shape["col"]),
        mesh=mesh,
        in_specs=(P("row", "col"), P("row", "col"), P("row", "col"), P(None, "row", "col"), P()),
        out_specs=(P(None, "row", "col"), P()),
        check_vma=False,
    )
```
